32 devices in a mesh: gx: 8 (over z, x), gy: 4 (over y, core).
Axes of the slice: x: 2, y: 2, z: 4, core: 2. Of those that a mesh axis runs over, the one named last changes fastest.
Arguments:
- source_tiles: bfloat16 [96, 32, 192, 384], P(('gx', 'gy')), may hold values from -6 to 6
- tile_offsets: int32 [2, 96], P(None, ('gx', 'gy')), may hold values from -128 to 896, as said below
- tile_shifts: int32 [96], P(('gx', 'gy')), may hold values from 0 to 63
- tile_counts: int32 [32], P(('gx', 'gy')), may hold values from 1 to 3, as said below
Outputs:
- merged_slab: float32 [32, 1024, 1024], P(None, 'gx', 'gy')
The draws below stay inside these ranges and needn't reach their ends.
Inputs may be any that keep to these rules, and one draw needn't show every extreme that they name: `tile_offsets`: slot k belongs to the device of joined gx+gy index d = k // 3, that is gx index d // 4 and gy index d % 4. Its x offset lies from that gx index times 128 minus 64 up to that gx index times 128; its y offset from the gy index times 256 minus 128 up to the gy index times 256. So every tile covers its owner's whole block. `tile_counts`: entry d counts the used slots of device d; they are its first slots, the others are ignored. Both 1 and 3 occur in every draw.
All inputs are finite; a program needn't handle non-finite values.
Results may differ from the reference program's by a relative error of at most 0.0003.
Values sent between devices are 32-bit elements; how exact they have to be, the bound alone decides.
A program may use at most 192 MiB of HBM per device.

```python
import jax
import jax.numpy as jnp
from jax import lax

NZ = 32
BX = 128
BY = 256
TX = 192
TY = 384
CAP = 3
RAMP = 32
NSHIFT = 64
RX = 64
RY = 128
NX = 1024
NY = 1024
TILES = 96


def draw_tile_offsets(key, part):
    holders = jnp.arange(TILES, dtype=jnp.int32) // CAP
    rows_gy = NY // BY
    column = holders // rows_gy
    row_place = holders % rows_gy
    key_x, key_y = jax.random.split(jax.random.fold_in(key, 11))
    back_x = jax.random.randint(key_x, (TILES,), 0, TX - BX + 1)
    back_y = jax.random.randint(key_y, (TILES,), 0, TY - BY + 1)
    back_x = back_x.at[0].set(TX - BX).at[TILES - 1].set(0)
    back_y = back_y.at[0].set(TY - BY).at[TILES - 1].set(0)
    return jnp.stack([column * BX - back_x, row_place * BY - back_y]).astype(jnp.int32)


def draw_tile_counts(key, part):
    counts = jax.random.randint(jax.random.fold_in(key, 23), (TILES // CAP,), 1, CAP + 1)
    counts = counts.at[0].set(CAP).at[1].set(1)
    return counts.astype(jnp.int32)


def plant(array, stream_key, smallest, top_value):
    longest = array.shape.index(max(array.shape))
    spots = []
    for shift in (0, 1):
        where = [jax.random.randint(jax.random.fold_in(stream_key, axis), (), 0, length) for axis, length in enumerate(array.shape)]
        where[longest] = (where[longest] + shift) % array.shape[longest]
        spots.append(tuple(where))
    return array.at[spots[0]].set(smallest).at[spots[1]].set(top_value)


def block_scale(rng, extent, shards, least, top_value):
    loudness = 1.0
    for dim, parts in shards:
        draws = jax.random.uniform(jax.random.fold_in(jax.random.fold_in(rng, 6), dim), (parts,), jnp.float32, least / len(shards), top_value / len(shards))
        loudness = loudness * jnp.repeat(jnp.exp(draws), extent[dim] // parts).reshape((-1,) + (1,) * (len(extent) - 1 - dim))
    return loudness


def noise(rng, extent, scale, bound, shards=(), kind=jnp.bfloat16):
    entries = scale * jax.random.normal(rng, extent, jnp.float32)
    if shards:
        entries = entries * block_scale(rng, extent, shards, -0.22, 0.18)
    return jnp.clip(entries, -bound, bound).astype(kind)


def setup_inputs(seed: int = 0) -> dict:
    streams_of = jax.random.split(jax.random.key(seed), 5)
    return {
        "source_tiles": noise(streams_of[0], (TILES, NZ, TX, TY), 1.0, 6.0, ((0, 32),)),
        "tile_offsets": draw_tile_offsets(jax.random.fold_in(streams_of[4], 71), 0),
        "tile_shifts": plant(jax.random.randint(streams_of[2], (TILES,), 0, NSHIFT), jax.random.fold_in(streams_of[2], 1), 0, NSHIFT - 1).astype(jnp.int32),
        "tile_counts": draw_tile_counts(jax.random.fold_in(streams_of[4], 71), 0),
    }


def interpolate(volume, fraction, dimension):
    length = volume.shape[dimension]
    shifted = jnp.concatenate([lax.slice_in_dim(volume, 1, length, axis=dimension), lax.slice_in_dim(volume, length - 1, length, axis=dimension)], axis=dimension)
    return (1.0 - fraction) * volume + fraction * shifted


def resample(source, shift_code):
    depth_part = ((shift_code // 16) % 4).astype(jnp.float32) * 0.25
    column_part = ((shift_code // 4) % 4).astype(jnp.float32) * 0.25
    row_part = (shift_code % 4).astype(jnp.float32) * 0.25
    volume = source.astype(jnp.float32)
    volume = interpolate(volume, depth_part, 0)
    volume = interpolate(volume, column_part, 1)
    return interpolate(volume, row_part, 2)


def blend_ramp(length):
    places = jnp.arange(length, dtype=jnp.float32)
    return jnp.minimum(jnp.minimum(places + 1.0, length - places), float(RAMP))


def reference(source_tiles, tile_offsets, tile_shifts, tile_counts):
    weight_plane = blend_ramp(TX)[:, None] * blend_ramp(TY)[None, :]
    values = jnp.zeros((NZ, NX + 2 * RX, NY + 2 * RY), jnp.float32)
    weights = jnp.zeros((NX + 2 * RX, NY + 2 * RY), jnp.float32)

    def place_tile(accumulated, number):
        values, weights = accumulated
        holder = number // CAP
        active = ((number % CAP) < tile_counts[holder]).astype(jnp.float32)
        source = lax.dynamic_index_in_dim(source_tiles, number, 0, keepdims=False)
        scaled = active * weight_plane
        volume = resample(source, tile_shifts[number]) * scaled[None]
        start_x = (tile_offsets[0, number] + RX).astype(jnp.int32)
        start_y = (tile_offsets[1, number] + RY).astype(jnp.int32)
        anchor = jnp.int32(0)
        window = lax.dynamic_slice(values, (anchor, start_x, start_y), (NZ, TX, TY))
        values = lax.dynamic_update_slice(values, window + volume, (anchor, start_x, start_y))
        weight_window = lax.dynamic_slice(weights, (start_x, start_y), (TX, TY))
        weights = lax.dynamic_update_slice(weights, weight_window + scaled, (start_x, start_y))
        return (values, weights), None

    (values, weights), ignored = lax.scan(place_tile, (values, weights), jnp.arange(TILES, dtype=jnp.int32))
    block_weights = weights[RX:RX + NX, RY:RY + NY]
    return values[:, RX:RX + NX, RY:RY + NY] / jnp.maximum(block_weights, 1.0)[None]
```

```python
import functools

import jax
import jax.numpy as jnp
from jax import lax
from jax.experimental import pallas as pl
from jax.experimental.pallas import tpu as pltpu
from jax.sharding import PartitionSpec as P

BX = 128
BY = 256
RAMP = 32
RX = 64
RY = 128
CHUNKS = 8


def passed_along(array, axis, by):
    count = lax.axis_size(axis)
    pairs = [(i, i + by) for i in range(count) if 0 <= i + by < count]
    return lax.ppermute(array, axis, pairs)


def ramp_at(place, length):
    place = place.astype(jnp.float32)
    ramp = jnp.minimum(jnp.minimum(place + 1.0, length - place), float(RAMP))
    return jnp.where((place >= 0) & (place < length), ramp, 0.0)


def band(starts, fractions, length, extent):
    target = jnp.arange(extent, dtype=jnp.int32)[None, :, None] - starts[:, None, None]
    source = jnp.arange(length, dtype=jnp.int32)[None, None, :]
    fraction = fractions[:, None, None]
    here = jnp.where(source == target, 1.0 - fraction, 0.0)
    after = jnp.where(source == jnp.minimum(target + 1, length - 1), fraction, 0.0)
    return ramp_at(target, length) * (here + after)


def tile_kernel(
    depth_ref, first_ref, next_ref, across_ref, along_ref, centre_ref, up_ref, down_ref, held, parts
):
    slots, length, rows = first_ref.shape[0], first_ref.shape[2], first_ref.shape[3]
    wide = along_ref.shape[2]
    half = wide // 2

    def along(plane, k):
        low = jnp.dot(plane, along_ref[k, :, :half], preferred_element_type=jnp.float32)
        cut = half - RY
        high = jnp.dot(
            plane[:, cut:], along_ref[k, cut:, half:], preferred_element_type=jnp.float32
        )
        return low, high

    @pl.when(pl.program_id(0) == 0)
    def _():
        for k in range(slots):
            low, high = along(first_ref[k, 0], k)
            held[k, :, :half] = low
            held[k, :, half:] = high

    for k in range(slots):
        fraction = depth_ref[k]
        for number, later in enumerate(along(next_ref[k, 0], k)):
            lanes = slice(number * half, (number + 1) * half)
            mixed = held[k, :, lanes] * (1.0 - fraction) + later * fraction
            held[k, :, lanes] = later
            top = mixed.astype(jnp.bfloat16)
            rest = (mixed - top.astype(jnp.float32)).astype(jnp.bfloat16)
            parts[2 * k * length : (2 * k + 1) * length, lanes] = top
            parts[(2 * k + 1) * length : (2 * k + 2) * length, lanes] = rest
    total = jnp.dot(across_ref[...], parts[...], preferred_element_type=jnp.float32)
    up_ref[0] = total[:, :RY]
    centre_ref[0] = total[:, RY : RY + BY]
    down_ref[0] = total[:, RY + BY :]


def place_tiles(chunk, depth, tiles, across, along, parts_of, dtype=jnp.float32):
    slots, depth_cells, length, rows = tiles.shape
    planes = depth_cells // CHUNKS
    begin = chunk * planes
    wide_x, wide_y = across.shape[0], along.shape[2]
    plane = (slots, 1, length, rows)
    return pl.pallas_call(
        tile_kernel,
        grid=(planes,),
        in_specs=[
            pl.BlockSpec(memory_space=pltpu.SMEM),
            pl.BlockSpec(plane, lambda z: (0, begin, 0, 0)),
            pl.BlockSpec(plane, lambda z: (0, jnp.minimum(begin + z + 1, depth_cells - 1), 0, 0)),
            pl.BlockSpec(across.shape, lambda z: (0, 0)),
            pl.BlockSpec(along.shape, lambda z: (0, 0, 0)),
        ],
        out_specs=[
            pl.BlockSpec((1, wide_x, BY), lambda z: (z, 0, 0)),
            pl.BlockSpec((1, wide_x, RY), lambda z: (z, 0, 0)),
            pl.BlockSpec((1, wide_x, RY), lambda z: (z, 0, 0)),
        ],
        out_shape=[
            jax.ShapeDtypeStruct((planes, wide_x, BY), dtype),
            jax.ShapeDtypeStruct((planes, wide_x, RY), dtype),
            jax.ShapeDtypeStruct((planes, wide_x, RY), dtype),
        ],
        scratch_shapes=[
            pltpu.VMEM((slots, length, wide_y), jnp.float32),
            pltpu.VMEM((2 * slots * length, wide_y), jnp.bfloat16),
        ],
        cost_estimate=pl.CostEstimate(
            flops=planes * 3_000_000_000 // 5, bytes_accessed=planes * 1_000_000, transcendentals=0
        ),
        name="place_tiles",
    )(depth, tiles, tiles, across, along)


def edge_kernel(left_ref, right_ref, below_l, above_l, below_r, above_r, to_left, to_right):
    for own, below, above, out in (
        (left_ref, below_l, above_l, to_left),
        (right_ref, below_r, above_r, to_right),
    ):
        out[:, :, :RY] = own[:, :, :RY] + below[...]
        out[:, :, RY:] = own[:, :, RY:] + above[...]


def edge_strips(centre, below, above):
    planes = centre.shape[0]
    last = (BX + RX) // RX
    wide = lambda place: pl.BlockSpec((planes, RX, BY), lambda i: (0, place, 0))
    slim = lambda place: pl.BlockSpec((planes, RX, RY), lambda i: (0, place, 0))
    shape = jax.ShapeDtypeStruct((planes, RX, BY), jnp.float32)
    return pl.pallas_call(
        edge_kernel,
        grid=(1,),
        in_specs=[wide(0), wide(last), slim(0), slim(0), slim(last), slim(last)],
        out_specs=[pl.BlockSpec((planes, RX, BY), lambda i: (0, 0, 0))] * 2,
        out_shape=[shape, shape],
        cost_estimate=pl.CostEstimate(
            flops=planes * RX * BY * 2, bytes_accessed=planes * RX * BY * 24, transcendentals=0
        ),
        name="edge_strips",
    )(centre, centre, below, above, below, above)


def merge_kernel(own_ref, below, above, from_side, scale, *rest):
    out = rest[-1]
    side = from_side[...]
    out[:, :, :RY] = (own_ref[:, :, :RY] + below[...] + side[:, :, :RY]) * scale[:, :RY][None]
    out[:, :, RY:] = (own_ref[:, :, RY:] + above[...] + side[:, :, RY:]) * scale[:, RY:][None]


def merge(chunk, half, depth_cells, centre, below, above, side, scale, previous):
    planes = centre.shape[0]
    start = RX // RX + half
    in_specs = [
        pl.BlockSpec((planes, RX, BY), lambda i: (0, start, 0)),
        pl.BlockSpec((planes, RX, RY), lambda i: (0, start, 0)),
        pl.BlockSpec((planes, RX, RY), lambda i: (0, start, 0)),
        pl.BlockSpec((planes, RX, BY), lambda i: (0, 0, 0)),
        pl.BlockSpec((RX, BY), lambda i: (half, 0)),
    ]
    operands = [centre, below, above, side, scale]
    aliases = {}
    if previous is not None:
        in_specs.append(pl.BlockSpec(memory_space=pl.ANY))
        operands.append(previous)
        aliases = {len(operands) - 1: 0}
    return pl.pallas_call(
        merge_kernel,
        grid=(1,),
        in_specs=in_specs,
        out_specs=pl.BlockSpec((planes, RX, BY), lambda i: (chunk, half, 0)),
        out_shape=jax.ShapeDtypeStruct((depth_cells, BX, BY), jnp.float32),
        input_output_aliases=aliases,
        cost_estimate=pl.CostEstimate(
            flops=planes * RX * BY * 3, bytes_accessed=planes * RX * BY * 16, transcendentals=0
        ),
        name="merge",
    )(*operands)


def block_scale(starts_x, starts_y, active):
    places = jnp.stack([starts_x - RX, starts_y - RY, active.astype(jnp.int32)])
    to_rows = jnp.array([0, BY, 0], jnp.int32)[:, None]
    to_columns = jnp.array([BX, 0, 0], jnp.int32)[:, None]
    places = jnp.concatenate(
        [
            places,
            passed_along(places, "gy", -1) + to_rows,
            passed_along(places, "gy", 1) - to_rows,
        ],
        axis=1,
    )
    return jnp.concatenate(
        [
            places,
            passed_along(places, "gx", -1) + to_columns,
            passed_along(places, "gx", 1) - to_columns,
        ],
        axis=1,
    )


def local(source_tiles, tile_offsets, tile_shifts, tile_counts):
    slots, depth_cells, length, rows = source_tiles.shape
    starts_x = tile_offsets[0] - lax.axis_index("gx") * BX + RX
    starts_y = tile_offsets[1] - lax.axis_index("gy") * BY + RY
    active = (jnp.arange(slots) < tile_counts[0]).astype(jnp.float32)
    depth_part = (tile_shifts // 16 % 4).astype(jnp.float32) * 0.25
    column_part = (tile_shifts // 4 % 4).astype(jnp.float32) * 0.25
    row_part = (tile_shifts % 4).astype(jnp.float32) * 0.25
    across = band(starts_x, column_part, length, BX + 2 * RX) * active[:, None, None]
    across = jnp.concatenate([across[k] for k in range(slots) for part in (0, 1)], axis=1)
    across = across.astype(jnp.bfloat16)
    along = band(starts_y, row_part, rows, BY + 2 * RY)
    along = jnp.swapaxes(along, 1, 2).astype(jnp.bfloat16)

    places = block_scale(starts_x, starts_y, active)
    x_ramps = ramp_at(jnp.arange(BX)[None, :] - places[0][:, None], length)
    x_ramps = x_ramps * places[2].astype(jnp.float32)[:, None]
    y_ramps = ramp_at(jnp.arange(BY)[None, :] - places[1][:, None], rows)
    weights = jnp.einsum("kx,ky->xy", x_ramps, y_ramps, precision=lax.Precision.HIGHEST)
    scale = 1.0 / jnp.maximum(weights, 1.0)

    out = None
    for chunk in range(CHUNKS):
        centre, up, down = place_tiles(
            chunk, depth_part, source_tiles, across, along, None
        )
        above = passed_along(up, "gy", -1)
        below = passed_along(down, "gy", 1)
        to_left, to_right = edge_strips(centre, below, above)
        from_right = passed_along(to_left, "gx", -1)
        from_left = passed_along(to_right, "gx", 1)
        out = merge(chunk, 0, depth_cells, centre, below, above, from_left, scale, out)
        out = merge(chunk, 1, depth_cells, centre, below, above, from_right, scale, out)
    return out


def solution(mesh):
    placed = (
        P(("gx", "gy"), None, None, None),
        P(None, ("gx", "gy")),
        P(("gx", "gy")),
        P(("gx", "gy")),
    )
    return jax.shard_map(
        local, mesh=mesh, in_specs=placed, out_specs=P(None, "gx", "gy"), check_vma=False
    )
```

```python
import functools

import jax
import jax.numpy as jnp
from jax import lax
from jax.experimental import pallas as pl
from jax.experimental.pallas import tpu as pltpu
from jax.sharding import PartitionSpec as P

BX = 128
BY = 256
RAMP = 32
RX = 64
RY = 128
LAG_Y = 2
LAG_X = 10
MESH = pl.DeviceIdType.MESH


def ramp_at(place, length):
    place = place.astype(jnp.float32)
    ramp = jnp.minimum(jnp.minimum(place + 1.0, length - place), float(RAMP))
    return jnp.where((place >= 0) & (place < length), ramp, 0.0)


def band(starts, fractions, length, extent):
    target = jnp.arange(extent, dtype=jnp.int32)[None, :, None] - starts[:, None, None]
    source = jnp.arange(length, dtype=jnp.int32)[None, None, :]
    fraction = fractions[:, None, None]
    here = jnp.where(source == target, 1.0 - fraction, 0.0)
    after = jnp.where(source == jnp.minimum(target + 1, length - 1), fraction, 0.0)
    return ramp_at(target, length) * (here + after)


def kernel(
    grid_x, grid_y, depth_ref, first_ref, next_ref, across_ref, along_ref, wide_x_ref, wide_y_ref,
    out_ref, centre, up, down, above, below, from_left, from_right, held, parts, scale,
    up_sent, down_sent, left_sent, right_sent, above_sem, below_sem, from_left_sem, from_right_sem,
):
    slots, length = first_ref.shape[0], first_ref.shape[2]
    half = along_ref.shape[2] // 2
    count = centre.shape[0]
    step = pl.program_id(0)
    column, row = lax.axis_index("gx"), lax.axis_index("gy")
    has_left, has_right = column > 0, column < grid_x - 1
    has_below, has_above = row > 0, row < grid_y - 1
    to_left, to_right = (column - 1, row), (column + 1, row)
    to_below, to_above = (column, row - 1), (column, row + 1)

    def remote(source, target, sent, arrived, device):
        return pltpu.make_async_remote_copy(
            src_ref=source, dst_ref=target, send_sem=sent, recv_sem=arrived,
            device_id=device, device_id_type=MESH,
        )

    def copy_below(n):
        return remote(up.at[n], above.at[n], up_sent.at[n], above_sem.at[n], to_below)

    def copy_above(n):
        return remote(down.at[n], below.at[n], down_sent.at[n], below_sem.at[n], to_above)

    def copy_left(n):
        return remote(
            centre.at[n, pl.ds(0, RX)], from_right.at[n], left_sent.at[n], from_right_sem.at[n], to_left
        )

    def copy_right(n):
        return remote(
            centre.at[n, pl.ds(RX + BX, RX)], from_left.at[n], right_sent.at[n], from_left_sem.at[n],
            to_right,
        )

    def along(plane, k):
        low = jnp.dot(plane, along_ref[k, :, :half], preferred_element_type=jnp.float32)
        cut = half - RY
        high = jnp.dot(
            plane[:, cut:], along_ref[k, cut:, half:], preferred_element_type=jnp.float32
        )
        return low, high

    def split(total):
        up[step] = total[:, :RY]
        centre[step] = total[:, RY : RY + BY]
        down[step] = total[:, RY + BY :]

    @pl.when(step == 0)
    def _():
        barrier = pltpu.get_barrier_semaphore()
        for there, device in (
            (has_left, to_left), (has_right, to_right), (has_below, to_below), (has_above, to_above)
        ):
            @pl.when(there)
            def _():
                pl.semaphore_signal(barrier, inc=1, device_id=device, device_id_type=MESH)

        split(jnp.dot(wide_x_ref[...], wide_y_ref[...], preferred_element_type=jnp.float32))
        for k in range(slots):
            low, high = along(first_ref[k, 0], k)
            held[k, :, :half] = low
            held[k, :, half:] = high
        peers = [jnp.where(there, 1, 0) for there in (has_left, has_right, has_below, has_above)]
        pl.semaphore_wait(barrier, sum(peers))

    @pl.when((step > 0) & (step < count))
    def _():
        for k in range(slots):
            fraction = depth_ref[k]
            for number, later in enumerate(along(next_ref[k, 0], k)):
                lanes = slice(number * half, (number + 1) * half)
                mixed = held[k, :, lanes] * (1.0 - fraction) + later * fraction
                held[k, :, lanes] = later
                top = mixed.astype(jnp.bfloat16)
                rest = (mixed - top.astype(jnp.float32)).astype(jnp.bfloat16)
                parts[2 * k * length : (2 * k + 1) * length, lanes] = top
                parts[(2 * k + 1) * length : (2 * k + 2) * length, lanes] = rest
        split(jnp.dot(across_ref[...], parts[...], preferred_element_type=jnp.float32))

    @pl.when(step < count)
    def _():
        @pl.when(has_below)
        def _():
            copy_below(step).start()

        @pl.when(has_above)
        def _():
            copy_above(step).start()

    @pl.when((step >= LAG_Y) & (step < count + LAG_Y))
    def _():
        n = step - LAG_Y

        @pl.when(has_below)
        def _():
            copy_above(n).wait_recv()
            centre[n, :, :RY] += below[n]

        @pl.when(has_above)
        def _():
            copy_below(n).wait_recv()
            centre[n, :, RY:] += above[n]

        @pl.when(has_left)
        def _():
            copy_left(n).start()

        @pl.when(has_right)
        def _():
            copy_right(n).start()

    @pl.when(step >= LAG_X)
    def _():
        n = step - LAG_X

        @pl.when(has_left)
        def _():
            copy_right(n).wait_recv()
            centre[n, RX : 2 * RX] += from_left[n]
            copy_left(n).wait_send()

        @pl.when(has_right)
        def _():
            copy_left(n).wait_recv()
            centre[n, BX : BX + RX] += from_right[n]
            copy_right(n).wait_send()

        @pl.when(has_below)
        def _():
            copy_below(n).wait_send()

        @pl.when(has_above)
        def _():
            copy_above(n).wait_send()

        @pl.when(n == 0)
        def _():
            scale[...] = 1.0 / jnp.maximum(centre[n, RX : RX + BX], 1.0)

        @pl.when(n > 0)
        def _():
            out_ref[0] = centre[n, RX : RX + BX] * scale[...]


def merged(grid_x, grid_y, depth, tiles, across, along, wide_x, wide_y):
    slots, depth_cells, length, rows = tiles.shape
    count = depth_cells + 1
    extent_x, extent_y = across.shape[0], along.shape[2]
    plane = (slots, 1, length, rows)
    slab = lambda *shape: pltpu.VMEM((count,) + shape, jnp.float32)
    return pl.pallas_call(
        functools.partial(kernel, grid_x, grid_y),
        grid=(count + LAG_X,),
        in_specs=[
            pl.BlockSpec(memory_space=pltpu.SMEM),
            pl.BlockSpec(plane, lambda s: (0, 0, 0, 0)),
            pl.BlockSpec(plane, lambda s: (0, jnp.clip(s, 1, depth_cells - 1), 0, 0)),
            pl.BlockSpec(across.shape, lambda s: (0, 0)),
            pl.BlockSpec(along.shape, lambda s: (0, 0, 0)),
            pl.BlockSpec(wide_x.shape, lambda s: (0, 0)),
            pl.BlockSpec(wide_y.shape, lambda s: (0, 0)),
        ],
        out_specs=pl.BlockSpec((1, BX, BY), lambda s: (jnp.maximum(s - LAG_X - 1, 0), 0, 0)),
        out_shape=jax.ShapeDtypeStruct((depth_cells, BX, BY), jnp.float32),
        scratch_shapes=[
            slab(extent_x, BY),
            slab(extent_x, RY),
            slab(extent_x, RY),
            slab(extent_x, RY),
            slab(extent_x, RY),
            slab(RX, BY),
            slab(RX, BY),
            pltpu.VMEM((slots, length, extent_y), jnp.float32),
            pltpu.VMEM((2 * slots * length, extent_y), jnp.bfloat16),
            pltpu.VMEM((BX, BY), jnp.float32),
        ]
        + [pltpu.SemaphoreType.DMA((count,))] * 8,
        compiler_params=pltpu.CompilerParams(
            collective_id=0, has_side_effects=True, vmem_limit_bytes=60 * 1024 * 1024,
            dimension_semantics=("arbitrary",),
        ),
        name="merged",
    )(depth, tiles, tiles, across, along, wide_x, wide_y)


def local(grid_x, grid_y, source_tiles, tile_offsets, tile_shifts, tile_counts):
    slots, depth_cells, length, rows = source_tiles.shape
    starts_x = tile_offsets[0] - lax.axis_index("gx") * BX + RX
    starts_y = tile_offsets[1] - lax.axis_index("gy") * BY + RY
    active = (jnp.arange(slots) < tile_counts[0]).astype(jnp.float32)
    depth_part = (tile_shifts // 16 % 4).astype(jnp.float32) * 0.25
    column_part = (tile_shifts // 4 % 4).astype(jnp.float32) * 0.25
    row_part = (tile_shifts % 4).astype(jnp.float32) * 0.25
    across = band(starts_x, column_part, length, BX + 2 * RX) * active[:, None, None]
    across = jnp.concatenate([across[k] for k in range(slots) for part in (0, 1)], axis=1)
    across = across.astype(jnp.bfloat16)
    along = band(starts_y, row_part, rows, BY + 2 * RY)
    along = jnp.swapaxes(along, 1, 2).astype(jnp.bfloat16)
    wide_x = ramp_at(jnp.arange(BX + 2 * RX)[:, None] - starts_x[None, :], length) * active[None, :]
    wide_y = ramp_at(jnp.arange(BY + 2 * RY)[None, :] - starts_y[:, None], rows)
    wide_x = jnp.pad(wide_x, ((0, 0), (0, 16 - slots))).astype(jnp.bfloat16)
    wide_y = jnp.pad(wide_y, ((0, 16 - slots), (0, 0))).astype(jnp.bfloat16)
    return merged(grid_x, grid_y, depth_part, source_tiles, across, along, wide_x, wide_y)


def solution(mesh):
    placed = (
        P(("gx", "gy"), None, None, None),
        P(None, ("gx", "gy")),
        P(("gx", "gy")),
        P(("gx", "gy")),
    )
    return jax.shard_map(
        functools.partial(local, mesh.shape["gx"], mesh.shape["gy"]),
        mesh=mesh, in_specs=placed, out_specs=P(None, "gx", "gy"), check_vma=False,
    )
```

```python
import functools

import jax
import jax.numpy as jnp
from jax import lax
from jax.experimental import pallas as pl
from jax.experimental.pallas import tpu as pltpu
from jax.sharding import PartitionSpec as P

BX = 128
BY = 256
RAMP = 32
RX = 64
RY = 128
LAG_Y = 2
LAG_RELAY = 6
LAG_X = 12
LANES = 128
MESH = pl.DeviceIdType.MESH


def ramp_at(place, length):
    place = place.astype(jnp.float32)
    ramp = jnp.minimum(jnp.minimum(place + 1.0, length - place), float(RAMP))
    return jnp.maximum(ramp, 0.0)


def whole_iota(shape, dimension):
    return lax.broadcasted_iota(jnp.int32, shape, dimension)


def pick(index, options):
    chosen = options[-1]
    for number in range(len(options) - 2, -1, -1):
        chosen = jnp.where(index == number, options[number], chosen)
    return chosen


def kernel(
    grid_x, grid_y, offsets_ref, shifts_ref, counts_ref, first_ref, next_ref,
    out_ref, centre, up, down, above, below, from_left, from_right, relay, places,
    across, along, held, parts, scale,
    up_sent, down_sent, left_sent, right_sent, above_sem, below_sem, from_left_sem, from_right_sem,
    relay_sent, relay_sem, place_sent, place_sem,
):
    slots, length, rows = first_ref.shape[0], first_ref.shape[2], first_ref.shape[3]
    extent_x, extent_y = across.shape[0], along.shape[2]
    half = extent_y // 2
    count = centre.shape[0]
    pairs = grid_x // 2
    step = pl.program_id(0)
    column, row = lax.axis_index("gx"), lax.axis_index("gy")
    even = column % 2 == 0
    pair = column // 2
    has_left, has_right = column > 0, column < grid_x - 1
    has_below, has_above = row > 0, row < grid_y - 1
    far_left, far_right = column > 1, column < grid_x - 2
    to_left, to_right = (column - 1, row), (column + 1, row)
    to_below, to_above = (column, row - 1), (column, row + 1)
    to_far_left, to_far_right = (column - 2, row), (column + 2, row)

    def remote(source, target, sent, arrived, device):
        return pltpu.make_async_remote_copy(
            src_ref=source, dst_ref=target, send_sem=sent, recv_sem=arrived,
            device_id=device, device_id_type=MESH,
        )

    def copy_below(n):
        return remote(up.at[n], above.at[n], up_sent.at[n], above_sem.at[n], to_below)

    def copy_above(n):
        return remote(down.at[n], below.at[n], down_sent.at[n], below_sem.at[n], to_above)

    left_strip, right_strip = pl.ds(0, RX), pl.ds(RX + BX, RX)

    def copy_left(n):
        return remote(
            centre.at[n, left_strip], from_right.at[n], left_sent.at[n], from_right_sem.at[n], to_left
        )

    def copy_right(n):
        return remote(
            centre.at[n, right_strip], from_left.at[n], right_sent.at[n], from_left_sem.at[n], to_right
        )

    def detour_left(n):
        return remote(
            centre.at[n, left_strip], relay.at[n], left_sent.at[n], relay_sem.at[n], to_right
        )

    def detour_right(n):
        return remote(
            centre.at[n, right_strip], relay.at[n], right_sent.at[n], relay_sem.at[n], to_left
        )

    def relay_left(n):
        return remote(relay.at[n], from_right.at[n], relay_sent.at[n], from_right_sem.at[n], to_far_left)

    def relay_right(n):
        return remote(relay.at[n], from_left.at[n], relay_sent.at[n], from_left_sem.at[n], to_far_right)

    def by_relay_right(n):
        return n % pairs < pairs - 1 - pair

    def by_relay_left(n):
        return n % pairs < pair

    def place_copy(first, size, target, number, device):
        return remote(
            places.at[pl.ds(first, size)], places.at[pl.ds(target, size)],
            place_sent.at[number], place_sem.at[number], device,
        )

    place_above = place_copy(0, 1, 1, 0, to_above)
    place_below = place_copy(0, 1, 2, 1, to_below)
    place_right = place_copy(0, 3, 3, 2, to_right)
    place_left = place_copy(0, 3, 6, 3, to_left)

    def along_rows(plane, k):
        low = jnp.dot(plane, along[k, :, :half], preferred_element_type=jnp.float32)
        cut = half - RY
        high = jnp.dot(plane[:, cut:], along[k, cut:, half:], preferred_element_type=jnp.float32)
        return low, high

    @pl.when(step == 0)
    def _():
        barrier = pltpu.get_barrier_semaphore()
        peers = (
            (has_left, to_left), (has_right, to_right), (has_below, to_below), (has_above, to_above),
            (far_left, to_far_left), (far_right, to_far_right),
        )
        for there, device in peers:
            @pl.when(there)
            def _():
                pl.semaphore_signal(barrier, inc=1, device_id=device, device_id_type=MESH)

        starts_x = [offsets_ref[0, k] - column * BX for k in range(slots)]
        starts_y = [offsets_ref[1, k] - row * BY for k in range(slots)]
        active = [jnp.where(k < counts_ref[0], 1.0, 0.0) for k in range(slots)]
        shape = places.shape[1:]
        lane, tile = whole_iota(shape, 1), whole_iota(shape, 0)
        record = jnp.zeros(shape, jnp.float32)
        for k in range(slots):
            values = (starts_x[k].astype(jnp.float32), starts_y[k].astype(jnp.float32), active[k])
            for place, value in enumerate(values):
                record = jnp.where((tile == k) & (lane == place), value, record)
        places[0] = record
        for number in range(1, places.shape[0]):
            there = (has_below, has_above, has_left, has_right)[
                number - 1 if number < 3 else number // 3 + 1
            ]

            @pl.when(jnp.logical_not(there))
            def _():
                places[number] = jnp.zeros(shape, jnp.float32)

        for k in range(slots):
            fraction = (shifts_ref[k] % 4).astype(jnp.float32) * 0.25
            target = whole_iota((1, extent_y), 1) - (starts_y[k] + RY)
            ramp = ramp_at(target, rows)
            source = whole_iota((rows, extent_y), 0)
            here = jnp.where(source == target, ramp * (1.0 - fraction), 0.0)
            after = jnp.where(
                source == jnp.minimum(target + 1, rows - 1), ramp * fraction, 0.0
            )
            along[k] = (here + after).astype(jnp.bfloat16)
        wide = 2 * slots * length
        number = whole_iota((1, wide), 1)
        part = number // length
        source = number - part * length
        part = part // 2
        fraction = pick(
            part, [(shifts_ref[k] // 4 % 4).astype(jnp.float32) * 0.25 for k in range(slots)]
        )
        weight = pick(part, active)
        target = whole_iota((extent_x, wide), 0) - pick(part, [start + RX for start in starts_x])
        here = jnp.where(source == target, 1.0 - fraction, 0.0)
        after = jnp.where(source == jnp.minimum(target + 1, length - 1), fraction, 0.0)
        across[...] = (ramp_at(target, length) * weight * (here + after)).astype(jnp.bfloat16)

        for k in range(slots):
            low, high = along_rows(first_ref[k, 0], k)
            held[k, :, :half] = low
            held[k, :, half:] = high
        pl.semaphore_wait(barrier, sum(jnp.where(there, 1, 0) for there, device in peers))

        @pl.when(has_above)
        def _():
            place_above.start()

        @pl.when(has_below)
        def _():
            place_below.start()

    @pl.when(step < count)
    def _():
        for k in range(slots):
            fraction = (shifts_ref[k] // 16 % 4).astype(jnp.float32) * 0.25
            for number, later in enumerate(along_rows(next_ref[k, 0], k)):
                lanes = slice(number * half, (number + 1) * half)
                mixed = held[k, :, lanes] * (1.0 - fraction) + later * fraction
                held[k, :, lanes] = later
                top = mixed.astype(jnp.bfloat16)
                rest = (mixed - top.astype(jnp.float32)).astype(jnp.bfloat16)
                parts[2 * k * length : (2 * k + 1) * length, lanes] = top
                parts[(2 * k + 1) * length : (2 * k + 2) * length, lanes] = rest
        total = jnp.dot(across[...], parts[...], preferred_element_type=jnp.float32)
        up[step] = total[:, :RY]
        centre[step] = total[:, RY : RY + BY]
        down[step] = total[:, RY + BY :]

        @pl.when(has_below)
        def _():
            copy_below(step).start()

        @pl.when(has_above)
        def _():
            copy_above(step).start()

    @pl.when(step == LAG_Y)
    def _():
        @pl.when(has_below)
        def _():
            place_above.wait_recv()

        @pl.when(has_above)
        def _():
            place_below.wait_recv()

        @pl.when(has_right)
        def _():
            place_right.start()

        @pl.when(has_left)
        def _():
            place_left.start()

    @pl.when((step >= LAG_Y) & (step < count + LAG_Y))
    def _():
        n = step - LAG_Y

        @pl.when(has_below)
        def _():
            copy_above(n).wait_recv()
            centre[n, :, :RY] += below[n]

        @pl.when(has_above)
        def _():
            copy_below(n).wait_recv()
            centre[n, :, RY:] += above[n]

        detours_left = even & by_relay_left(n)
        detours_right = jnp.logical_not(even) & by_relay_right(n)

        @pl.when(has_left & detours_left)
        def _():
            detour_left(n).start()

        @pl.when(has_left & jnp.logical_not(detours_left))
        def _():
            copy_left(n).start()

        @pl.when(has_right & detours_right)
        def _():
            detour_right(n).start()

        @pl.when(has_right & jnp.logical_not(detours_right))
        def _():
            copy_right(n).start()

    @pl.when((step >= LAG_RELAY) & (step < count + LAG_RELAY))
    def _():
        n = step - LAG_RELAY

        @pl.when(even & far_right & by_relay_right(n))
        def _():
            detour_right(n).wait_recv()
            relay_right(n).start()

        @pl.when(jnp.logical_not(even) & far_left & by_relay_left(n))
        def _():
            detour_left(n).wait_recv()
            relay_left(n).start()

    @pl.when(step == LAG_X)
    def _():
        for there, copy in ((has_above, place_above), (has_below, place_below)):
            @pl.when(there)
            def _():
                copy.wait_send()

        @pl.when(has_left)
        def _():
            place_right.wait_recv()
            place_left.wait_send()

        @pl.when(has_right)
        def _():
            place_left.wait_recv()
            place_right.wait_send()

        total = jnp.zeros((BX, BY), jnp.float32)
        cell_x = whole_iota((BX, 1), 0).astype(jnp.float32)
        cell_y = whole_iota((1, BY), 1).astype(jnp.float32)
        for number in range(places.shape[0]):
            origin_x = float((0, -BX, BX)[number // 3])
            origin_y = float((0, -BY, BY)[number % 3])
            for k in range(slots):
                start_x = places[number, k : k + 1, 0:1] + origin_x
                start_y = places[number, k : k + 1, 1:2] + origin_y
                weight = places[number, k : k + 1, 2:3]
                total += (ramp_at(cell_x - start_x, length) * weight) * ramp_at(cell_y - start_y, rows)
        scale[...] = 1.0 / jnp.maximum(total, 1.0)

    @pl.when(step >= LAG_X)
    def _():
        n = step - LAG_X

        @pl.when(has_left)
        def _():
            copy_right(n).wait_recv()
            centre[n, RX : 2 * RX] += from_left[n]
            copy_left(n).wait_send()

        @pl.when(has_right)
        def _():
            copy_left(n).wait_recv()
            centre[n, BX : BX + RX] += from_right[n]
            copy_right(n).wait_send()

        @pl.when(has_below)
        def _():
            copy_below(n).wait_send()

        @pl.when(has_above)
        def _():
            copy_above(n).wait_send()

        @pl.when(even & far_right & by_relay_right(n))
        def _():
            relay_right(n).wait_send()

        @pl.when(jnp.logical_not(even) & far_left & by_relay_left(n))
        def _():
            relay_left(n).wait_send()

        out_ref[0] = centre[n, RX : RX + BX] * scale[...]


def local(grid_x, grid_y, tiles, tile_offsets, tile_shifts, tile_counts):
    slots, count, length, rows = tiles.shape
    extent_x, extent_y = BX + 2 * RX, BY + 2 * RY
    plane = (slots, 1, length, rows)
    slab = lambda *shape: pltpu.VMEM((count,) + shape, jnp.float32)
    return pl.pallas_call(
        functools.partial(kernel, grid_x, grid_y),
        grid=(count + LAG_X,),
        in_specs=[
            pl.BlockSpec(memory_space=pltpu.SMEM),
            pl.BlockSpec(memory_space=pltpu.SMEM),
            pl.BlockSpec(memory_space=pltpu.SMEM),
            pl.BlockSpec(plane, lambda s: (0, 0, 0, 0)),
            pl.BlockSpec(plane, lambda s: (0, jnp.minimum(s + 1, count - 1), 0, 0)),
        ],
        out_specs=pl.BlockSpec((1, BX, BY), lambda s: (jnp.maximum(s - LAG_X, 0), 0, 0)),
        out_shape=jax.ShapeDtypeStruct((count, BX, BY), jnp.float32),
        scratch_shapes=[
            slab(extent_x, BY),
            slab(extent_x, RY),
            slab(extent_x, RY),
            slab(extent_x, RY),
            slab(extent_x, RY),
            slab(RX, BY),
            slab(RX, BY),
            slab(RX, BY),
            pltpu.VMEM((9, 8 * pl.cdiv(slots, 8), LANES), jnp.float32),
            pltpu.VMEM((extent_x, 2 * slots * length), jnp.bfloat16),
            pltpu.VMEM((slots, rows, extent_y), jnp.bfloat16),
            pltpu.VMEM((slots, length, extent_y), jnp.float32),
            pltpu.VMEM((2 * slots * length, extent_y), jnp.bfloat16),
            pltpu.VMEM((BX, BY), jnp.float32),
        ]
        + [pltpu.SemaphoreType.DMA((count,))] * 10
        + [pltpu.SemaphoreType.DMA((4,))] * 2,
        compiler_params=pltpu.CompilerParams(
            collective_id=0, has_side_effects=True, vmem_limit_bytes=60 * 1024 * 1024,
            dimension_semantics=("arbitrary",),
        ),
        name="merged",
    )(tile_offsets, tile_shifts, tile_counts, tiles, tiles)


def solution(mesh):
    placed = (
        P(("gx", "gy"), None, None, None),
        P(None, ("gx", "gy")),
        P(("gx", "gy")),
        P(("gx", "gy")),
    )
    return jax.shard_map(
        functools.partial(local, mesh.shape["gx"], mesh.shape["gy"]),
        mesh=mesh, in_specs=placed, out_specs=P(None, "gx", "gy"), check_vma=False,
    )
```

```python
import functools

import jax
import jax.numpy as jnp
from jax import lax
from jax.experimental import pallas as pl
from jax.experimental.pallas import tpu as pltpu
from jax.sharding import PartitionSpec as P

BX = 128
BY = 256
RAMP = 32
RX = 64
RY = 128
LAG_Y = 1
LAG_RELAY = 5
LAG_X = 12
LANES = 128
MESH = pl.DeviceIdType.MESH


def ramp_at(place, length):
    place = place.astype(jnp.float32)
    ramp = jnp.minimum(jnp.minimum(place + 1.0, length - place), float(RAMP))
    return jnp.maximum(ramp, 0.0)


def whole_iota(shape, dimension):
    return lax.broadcasted_iota(jnp.int32, shape, dimension)


def pick(index, options):
    chosen = options[-1]
    for number in range(len(options) - 2, -1, -1):
        chosen = jnp.where(index == number, options[number], chosen)
    return chosen


def kernel(
    grid_x, grid_y, offsets_ref, shifts_ref, counts_ref, first_ref, next_ref,
    out_ref, centre, up, down, above, below, from_left, from_right, relay, places,
    across, along, held, parts, scale,
    up_sent, down_sent, left_sent, right_sent, above_sem, below_sem, from_left_sem, from_right_sem,
    relay_sent, relay_sem, place_sent, place_sem,
):
    slots, length, rows = first_ref.shape[0], first_ref.shape[2], first_ref.shape[3]
    extent_x, extent_y = across.shape[0], along.shape[2]
    half = extent_y // 2
    count = centre.shape[0]
    pairs = grid_x // 2
    step = pl.program_id(0)
    column, row = lax.axis_index("gx"), lax.axis_index("gy")
    even = column % 2 == 0
    pair = column // 2
    has_left, has_right = column > 0, column < grid_x - 1
    has_below, has_above = row > 0, row < grid_y - 1
    far_left, far_right = column > 1, column < grid_x - 2
    to_left, to_right = (column - 1, row), (column + 1, row)
    to_below, to_above = (column, row - 1), (column, row + 1)
    to_far_left, to_far_right = (column - 2, row), (column + 2, row)

    def remote(source, target, sent, arrived, device):
        return pltpu.make_async_remote_copy(
            src_ref=source, dst_ref=target, send_sem=sent, recv_sem=arrived,
            device_id=device, device_id_type=MESH,
        )

    def copy_below(n):
        return remote(up.at[n], above.at[n], up_sent.at[n], above_sem.at[n], to_below)

    def copy_above(n):
        return remote(down.at[n], below.at[n], down_sent.at[n], below_sem.at[n], to_above)

    left_strip, right_strip = pl.ds(0, RX), pl.ds(RX + BX, RX)

    def copy_left(n):
        return remote(
            centre.at[n, left_strip], from_right.at[n], left_sent.at[n], from_right_sem.at[n], to_left
        )

    def copy_right(n):
        return remote(
            centre.at[n, right_strip], from_left.at[n], right_sent.at[n], from_left_sem.at[n], to_right
        )

    def detour_left(n):
        return remote(
            centre.at[n, left_strip], relay.at[n], left_sent.at[n], relay_sem.at[n], to_right
        )

    def detour_right(n):
        return remote(
            centre.at[n, right_strip], relay.at[n], right_sent.at[n], relay_sem.at[n], to_left
        )

    def relay_left(n):
        return remote(relay.at[n], from_right.at[n], relay_sent.at[n], from_right_sem.at[n], to_far_left)

    def relay_right(n):
        return remote(relay.at[n], from_left.at[n], relay_sent.at[n], from_left_sem.at[n], to_far_right)

    def by_relay_right(n):
        return n % pairs < pairs - 1 - pair

    def by_relay_left(n):
        return n % pairs < pair

    def place_copy(first, size, target, number, device):
        return remote(
            places.at[pl.ds(first, size)], places.at[pl.ds(target, size)],
            place_sent.at[number], place_sem.at[number], device,
        )

    place_above = place_copy(0, 1, 1, 0, to_above)
    place_below = place_copy(0, 1, 2, 1, to_below)
    place_right = place_copy(0, 3, 3, 2, to_right)
    place_left = place_copy(0, 3, 6, 3, to_left)

    def along_rows(plane, k):
        low = jnp.dot(plane, along[k, :, :half], preferred_element_type=jnp.float32)
        cut = half - RY
        high = jnp.dot(plane[:, cut:], along[k, cut:, half:], preferred_element_type=jnp.float32)
        return low, high

    @pl.when(step == 0)
    def _():
        barrier = pltpu.get_barrier_semaphore()
        peers = (
            (has_left, to_left), (has_right, to_right), (has_below, to_below), (has_above, to_above),
            (far_left, to_far_left), (far_right, to_far_right),
        )
        for there, device in peers:
            @pl.when(there)
            def _():
                pl.semaphore_signal(barrier, inc=1, device_id=device, device_id_type=MESH)

        starts_x = [offsets_ref[0, k] - column * BX for k in range(slots)]
        starts_y = [offsets_ref[1, k] - row * BY for k in range(slots)]
        active = [jnp.where(k < counts_ref[0], 1.0, 0.0) for k in range(slots)]
        shape = places.shape[1:]
        lane, tile = whole_iota(shape, 1), whole_iota(shape, 0)
        record = jnp.zeros(shape, jnp.float32)
        for k in range(slots):
            values = (starts_x[k].astype(jnp.float32), starts_y[k].astype(jnp.float32), active[k])
            for place, value in enumerate(values):
                record = jnp.where((tile == k) & (lane == place), value, record)
        places[0] = record
        for number in range(1, places.shape[0]):
            there = (has_below, has_above, has_left, has_right)[
                number - 1 if number < 3 else number // 3 + 1
            ]

            @pl.when(jnp.logical_not(there))
            def _():
                places[number] = jnp.zeros(shape, jnp.float32)

        for k in range(slots):
            fraction = (shifts_ref[k] % 4).astype(jnp.float32) * 0.25
            target = whole_iota((1, extent_y), 1) - (starts_y[k] + RY)
            ramp = ramp_at(target, rows)
            source = whole_iota((rows, extent_y), 0)
            here = jnp.where(source == target, ramp * (1.0 - fraction), 0.0)
            after = jnp.where(
                source == jnp.minimum(target + 1, rows - 1), ramp * fraction, 0.0
            )
            along[k] = (here + after).astype(jnp.bfloat16)
        wide = 2 * slots * length
        number = whole_iota((1, wide), 1)
        part = number // length
        source = number - part * length
        part = part // 2
        fraction = pick(
            part, [(shifts_ref[k] // 4 % 4).astype(jnp.float32) * 0.25 for k in range(slots)]
        )
        weight = pick(part, active)
        target = whole_iota((extent_x, wide), 0) - pick(part, [start + RX for start in starts_x])
        here = jnp.where(source == target, 1.0 - fraction, 0.0)
        after = jnp.where(source == jnp.minimum(target + 1, length - 1), fraction, 0.0)
        across[...] = (ramp_at(target, length) * weight * (here + after)).astype(jnp.bfloat16)

        for k in range(slots):
            low, high = along_rows(first_ref[k, 0], k)
            held[k, :, :half] = low
            held[k, :, half:] = high
        pl.semaphore_wait(barrier, sum(jnp.where(there, 1, 0) for there, device in peers))

        @pl.when(has_above)
        def _():
            place_above.start()

        @pl.when(has_below)
        def _():
            place_below.start()

    @pl.when(step < count)
    def _():
        for k in range(slots):
            fraction = (shifts_ref[k] // 16 % 4).astype(jnp.float32) * 0.25
            for number, later in enumerate(along_rows(next_ref[k, 0], k)):
                lanes = slice(number * half, (number + 1) * half)
                mixed = held[k, :, lanes] * (1.0 - fraction) + later * fraction
                held[k, :, lanes] = later
                top = mixed.astype(jnp.bfloat16)
                rest = (mixed - top.astype(jnp.float32)).astype(jnp.bfloat16)
                parts[2 * k * length : (2 * k + 1) * length, lanes] = top
                parts[(2 * k + 1) * length : (2 * k + 2) * length, lanes] = rest
        total = jnp.dot(across[...], parts[...], preferred_element_type=jnp.float32)
        up[step] = total[:, :RY]
        centre[step] = total[:, RY : RY + BY]
        down[step] = total[:, RY + BY :]

        @pl.when(has_below)
        def _():
            copy_below(step).start()

        @pl.when(has_above)
        def _():
            copy_above(step).start()

    @pl.when(step == LAG_Y)
    def _():
        @pl.when(has_below)
        def _():
            place_above.wait_recv()

        @pl.when(has_above)
        def _():
            place_below.wait_recv()

        @pl.when(has_right)
        def _():
            place_right.start()

        @pl.when(has_left)
        def _():
            place_left.start()

    @pl.when((step >= LAG_Y) & (step < count + LAG_Y))
    def _():
        n = step - LAG_Y

        @pl.when(has_below)
        def _():
            copy_above(n).wait_recv()
            centre[n, :, :RY] += below[n]

        @pl.when(has_above)
        def _():
            copy_below(n).wait_recv()
            centre[n, :, RY:] += above[n]

        detours_left = even & by_relay_left(n)
        detours_right = jnp.logical_not(even) & by_relay_right(n)

        @pl.when(has_left & detours_left)
        def _():
            detour_left(n).start()

        @pl.when(has_left & jnp.logical_not(detours_left))
        def _():
            copy_left(n).start()

        @pl.when(has_right & detours_right)
        def _():
            detour_right(n).start()

        @pl.when(has_right & jnp.logical_not(detours_right))
        def _():
            copy_right(n).start()

    @pl.when((step >= LAG_RELAY) & (step < count + LAG_RELAY))
    def _():
        n = step - LAG_RELAY

        @pl.when(even & far_right & by_relay_right(n))
        def _():
            detour_right(n).wait_recv()
            relay_right(n).start()

        @pl.when(jnp.logical_not(even) & far_left & by_relay_left(n))
        def _():
            detour_left(n).wait_recv()
            relay_left(n).start()

    @pl.when(step == LAG_X)
    def _():
        for there, copy in ((has_above, place_above), (has_below, place_below)):
            @pl.when(there)
            def _():
                copy.wait_send()

        @pl.when(has_left)
        def _():
            place_right.wait_recv()
            place_left.wait_send()

        @pl.when(has_right)
        def _():
            place_left.wait_recv()
            place_right.wait_send()

        total = jnp.zeros((BX, BY), jnp.float32)
        cell_x = whole_iota((BX, 1), 0).astype(jnp.float32)
        cell_y = whole_iota((1, BY), 1).astype(jnp.float32)
        for number in range(places.shape[0]):
            origin_x = float((0, -BX, BX)[number // 3])
            origin_y = float((0, -BY, BY)[number % 3])
            for k in range(slots):
                start_x = places[number, k : k + 1, 0:1] + origin_x
                start_y = places[number, k : k + 1, 1:2] + origin_y
                weight = places[number, k : k + 1, 2:3]
                total += (ramp_at(cell_x - start_x, length) * weight) * ramp_at(cell_y - start_y, rows)
        scale[...] = 1.0 / jnp.maximum(total, 1.0)

    @pl.when(step >= LAG_X)
    def _():
        n = step - LAG_X

        @pl.when(has_left)
        def _():
            copy_right(n).wait_recv()
            centre[n, RX : 2 * RX] += from_left[n]
            copy_left(n).wait_send()

        @pl.when(has_right)
        def _():
            copy_left(n).wait_recv()
            centre[n, BX : BX + RX] += from_right[n]
            copy_right(n).wait_send()

        @pl.when(has_below)
        def _():
            copy_below(n).wait_send()

        @pl.when(has_above)
        def _():
            copy_above(n).wait_send()

        @pl.when(even & far_right & by_relay_right(n))
        def _():
            relay_right(n).wait_send()

        @pl.when(jnp.logical_not(even) & far_left & by_relay_left(n))
        def _():
            relay_left(n).wait_send()

        out_ref[n] = centre[n, RX : RX + BX] * scale[...]


def local(grid_x, grid_y, tiles, tile_offsets, tile_shifts, tile_counts):
    slots, count, length, rows = tiles.shape
    extent_x, extent_y = BX + 2 * RX, BY + 2 * RY
    plane = (slots, 1, length, rows)
    slab = lambda *shape: pltpu.VMEM((count,) + shape, jnp.float32)
    return pl.pallas_call(
        functools.partial(kernel, grid_x, grid_y),
        grid=(count + LAG_X,),
        in_specs=[
            pl.BlockSpec(memory_space=pltpu.SMEM),
            pl.BlockSpec(memory_space=pltpu.SMEM),
            pl.BlockSpec(memory_space=pltpu.SMEM),
            pl.BlockSpec(plane, lambda s: (0, 0, 0, 0)),
            pl.BlockSpec(plane, lambda s: (0, jnp.minimum(s + 1, count - 1), 0, 0)),
        ],
        out_specs=pl.BlockSpec(memory_space=pltpu.VMEM),
        out_shape=pltpu.VMEM((count, BX, BY), jnp.float32),
        scratch_shapes=[
            slab(extent_x, BY),
            slab(extent_x, RY),
            slab(extent_x, RY),
            slab(extent_x, RY),
            slab(extent_x, RY),
            slab(RX, BY),
            slab(RX, BY),
            slab(RX, BY),
            pltpu.VMEM((9, 8 * pl.cdiv(slots, 8), LANES), jnp.float32),
            pltpu.VMEM((extent_x, 2 * slots * length), jnp.bfloat16),
            pltpu.VMEM((slots, rows, extent_y), jnp.bfloat16),
            pltpu.VMEM((slots, length, extent_y), jnp.float32),
            pltpu.VMEM((2 * slots * length, extent_y), jnp.bfloat16),
            pltpu.VMEM((BX, BY), jnp.float32),
        ]
        + [pltpu.SemaphoreType.DMA((count,))] * 10
        + [pltpu.SemaphoreType.DMA((4,))] * 2,
        compiler_params=pltpu.CompilerParams(
            collective_id=0, has_side_effects=True, vmem_limit_bytes=52 * 1024 * 1024,
            dimension_semantics=("arbitrary",),
        ),
        name="merged",
    )(tile_offsets, tile_shifts, tile_counts, tiles, tiles)


def solution(mesh):
    placed = (
        P(("gx", "gy"), None, None, None),
        P(None, ("gx", "gy")),
        P(("gx", "gy")),
        P(("gx", "gy")),
    )
    return jax.shard_map(
        functools.partial(local, mesh.shape["gx"], mesh.shape["gy"]),
        mesh=mesh, in_specs=placed, out_specs=P(None, "gx", "gy"), check_vma=False,
    )
```

```python
import functools

import jax
import jax.numpy as jnp
from jax import lax
from jax.experimental import pallas as pl
from jax.experimental.pallas import tpu as pltpu
from jax.sharding import PartitionSpec as P

BX = 128
BY = 256
RAMP = 32
RX = 64
RY = 128
LAG_Y = 1
LAG_RELAY = 5
LAG_X = 12
LANES = 128
MESH = pl.DeviceIdType.MESH


def ramp_at(place, length):
    place = place.astype(jnp.float32)
    ramp = jnp.minimum(jnp.minimum(place + 1.0, length - place), float(RAMP))
    return jnp.maximum(ramp, 0.0)


def whole_iota(shape, dimension):
    return lax.broadcasted_iota(jnp.int32, shape, dimension)


def kernel(
    grid_x, grid_y, offsets_ref, shifts_ref, counts_ref, first_ref, next_ref,
    out_ref, centre, up, down, above, below, from_left, from_right, relay, places,
    across, along, held, parts, scale,
    up_sent, down_sent, left_sent, right_sent, above_sem, below_sem, from_left_sem, from_right_sem,
    relay_sent, relay_sem, place_sent, place_sem,
):
    slots, length, rows = first_ref.shape[0], first_ref.shape[2], first_ref.shape[3]
    extent_x, extent_y = across.shape[0], along.shape[2]
    half = extent_y // 2
    count = centre.shape[0]
    pairs = grid_x // 2
    step = pl.program_id(0)
    column, row = lax.axis_index("gx"), lax.axis_index("gy")
    even = column % 2 == 0
    pair = column // 2
    has_left, has_right = column > 0, column < grid_x - 1
    has_below, has_above = row > 0, row < grid_y - 1
    far_left, far_right = column > 1, column < grid_x - 2
    to_left, to_right = (column - 1, row), (column + 1, row)
    to_below, to_above = (column, row - 1), (column, row + 1)
    to_far_left, to_far_right = (column - 2, row), (column + 2, row)

    def remote(source, target, sent, arrived, device):
        return pltpu.make_async_remote_copy(
            src_ref=source, dst_ref=target, send_sem=sent, recv_sem=arrived,
            device_id=device, device_id_type=MESH,
        )

    def copy_below(n):
        return remote(up.at[n], above.at[n], up_sent.at[n], above_sem.at[n], to_below)

    def copy_above(n):
        return remote(down.at[n], below.at[n], down_sent.at[n], below_sem.at[n], to_above)

    left_strip, right_strip = pl.ds(0, RX), pl.ds(RX + BX, RX)

    def copy_left(n):
        return remote(
            centre.at[n, left_strip], from_right.at[n], left_sent.at[n], from_right_sem.at[n], to_left
        )

    def copy_right(n):
        return remote(
            centre.at[n, right_strip], from_left.at[n], right_sent.at[n], from_left_sem.at[n], to_right
        )

    def detour_left(n):
        return remote(
            centre.at[n, left_strip], relay.at[n], left_sent.at[n], relay_sem.at[n], to_right
        )

    def detour_right(n):
        return remote(
            centre.at[n, right_strip], relay.at[n], right_sent.at[n], relay_sem.at[n], to_left
        )

    def relay_left(n):
        return remote(relay.at[n], from_right.at[n], relay_sent.at[n], from_right_sem.at[n], to_far_left)

    def relay_right(n):
        return remote(relay.at[n], from_left.at[n], relay_sent.at[n], from_left_sem.at[n], to_far_right)

    def by_relay_right(n):
        return n % pairs < pairs - 1 - pair

    def by_relay_left(n):
        return n % pairs < pair

    def place_copy(first, size, target, number, device):
        return remote(
            places.at[pl.ds(first, size)], places.at[pl.ds(target, size)],
            place_sent.at[number], place_sem.at[number], device,
        )

    place_above = place_copy(0, 1, 1, 0, to_above)
    place_below = place_copy(0, 1, 2, 1, to_below)
    place_right = place_copy(0, 3, 3, 2, to_right)
    place_left = place_copy(0, 3, 6, 3, to_left)

    def along_rows(plane, k):
        low = jnp.dot(plane, along[k, :, :half], preferred_element_type=jnp.float32)
        cut = half - RY
        high = jnp.dot(plane[:, cut:], along[k, cut:, half:], preferred_element_type=jnp.float32)
        return low, high

    @pl.when(step == 0)
    def _():
        barrier = pltpu.get_barrier_semaphore()
        peers = (
            (has_left, to_left), (has_right, to_right), (has_below, to_below), (has_above, to_above),
            (far_left, to_far_left), (far_right, to_far_right),
        )
        for there, device in peers:
            @pl.when(there)
            def _():
                pl.semaphore_signal(barrier, inc=1, device_id=device, device_id_type=MESH)

        starts_x = [offsets_ref[0, k] - column * BX for k in range(slots)]
        starts_y = [offsets_ref[1, k] - row * BY for k in range(slots)]
        active = [jnp.where(k < counts_ref[0], 1.0, 0.0) for k in range(slots)]
        shape = places.shape[1:]
        lane, tile = whole_iota(shape, 1), whole_iota(shape, 0)
        record = jnp.zeros(shape, jnp.float32)
        for k in range(slots):
            values = (starts_x[k].astype(jnp.float32), starts_y[k].astype(jnp.float32), active[k])
            for place, value in enumerate(values):
                record = jnp.where((tile == k) & (lane == place), value, record)
        places[0] = record
        for number in range(1, places.shape[0]):
            there = (has_below, has_above, has_left, has_right)[
                number - 1 if number < 3 else number // 3 + 1
            ]

            @pl.when(jnp.logical_not(there))
            def _():
                places[number] = jnp.zeros(shape, jnp.float32)

        for k in range(slots):
            fraction = (shifts_ref[k] % 4).astype(jnp.float32) * 0.25
            target = whole_iota((1, extent_y), 1) - (starts_y[k] + RY)
            ramp = ramp_at(target, rows)
            source = whole_iota((rows, extent_y), 0)
            here = jnp.where(source == target, ramp * (1.0 - fraction), 0.0)
            after = jnp.where(
                source == jnp.minimum(target + 1, rows - 1), ramp * fraction, 0.0
            )
            along[k] = (here + after).astype(jnp.bfloat16)
        for k in range(slots):
            fraction = (shifts_ref[k] // 4 % 4).astype(jnp.float32) * 0.25
            target = whole_iota((extent_x, 1), 0) - (starts_x[k] + RX)
            ramp = ramp_at(target, length) * active[k]
            source = whole_iota((extent_x, length), 1)
            here = jnp.where(source == target, ramp * (1.0 - fraction), 0.0)
            after = jnp.where(
                source == jnp.minimum(target + 1, length - 1), ramp * fraction, 0.0
            )
            placed = (here + after).astype(jnp.bfloat16)
            across[:, 2 * k * length : (2 * k + 1) * length] = placed
            across[:, (2 * k + 1) * length : (2 * k + 2) * length] = placed

        for k in range(slots):
            low, high = along_rows(first_ref[k, 0], k)
            held[k, :, :half] = low
            held[k, :, half:] = high
        pl.semaphore_wait(barrier, sum(jnp.where(there, 1, 0) for there, device in peers))

        @pl.when(has_above)
        def _():
            place_above.start()

        @pl.when(has_below)
        def _():
            place_below.start()

    @pl.when(step < count)
    def _():
        for k in range(slots):
            fraction = (shifts_ref[k] // 16 % 4).astype(jnp.float32) * 0.25
            for number, later in enumerate(along_rows(next_ref[k, 0], k)):
                lanes = slice(number * half, (number + 1) * half)
                mixed = held[k, :, lanes] * (1.0 - fraction) + later * fraction
                held[k, :, lanes] = later
                top = mixed.astype(jnp.bfloat16)
                rest = (mixed - top.astype(jnp.float32)).astype(jnp.bfloat16)
                parts[2 * k * length : (2 * k + 1) * length, lanes] = top
                parts[(2 * k + 1) * length : (2 * k + 2) * length, lanes] = rest
        total = jnp.dot(across[...], parts[...], preferred_element_type=jnp.float32)
        up[step] = total[:, :RY]
        centre[step] = total[:, RY : RY + BY]
        down[step] = total[:, RY + BY :]

        @pl.when(has_below)
        def _():
            copy_below(step).start()

        @pl.when(has_above)
        def _():
            copy_above(step).start()

    @pl.when(step == LAG_Y)
    def _():
        @pl.when(has_below)
        def _():
            place_above.wait_recv()

        @pl.when(has_above)
        def _():
            place_below.wait_recv()

        @pl.when(has_right)
        def _():
            place_right.start()

        @pl.when(has_left)
        def _():
            place_left.start()

    @pl.when((step >= LAG_Y) & (step < count + LAG_Y))
    def _():
        n = step - LAG_Y

        @pl.when(has_below)
        def _():
            copy_above(n).wait_recv()
            centre[n, :, :RY] += below[n]

        @pl.when(has_above)
        def _():
            copy_below(n).wait_recv()
            centre[n, :, RY:] += above[n]

        detours_left = even & by_relay_left(n)
        detours_right = jnp.logical_not(even) & by_relay_right(n)

        @pl.when(has_left & detours_left)
        def _():
            detour_left(n).start()

        @pl.when(has_left & jnp.logical_not(detours_left))
        def _():
            copy_left(n).start()

        @pl.when(has_right & detours_right)
        def _():
            detour_right(n).start()

        @pl.when(has_right & jnp.logical_not(detours_right))
        def _():
            copy_right(n).start()

    @pl.when((step >= LAG_RELAY) & (step < count + LAG_RELAY))
    def _():
        n = step - LAG_RELAY

        @pl.when(even & far_right & by_relay_right(n))
        def _():
            detour_right(n).wait_recv()
            relay_right(n).start()

        @pl.when(jnp.logical_not(even) & far_left & by_relay_left(n))
        def _():
            detour_left(n).wait_recv()
            relay_left(n).start()

    @pl.when(step == LAG_X)
    def _():
        for there, copy in ((has_above, place_above), (has_below, place_below)):
            @pl.when(there)
            def _():
                copy.wait_send()

        @pl.when(has_left)
        def _():
            place_right.wait_recv()
            place_left.wait_send()

        @pl.when(has_right)
        def _():
            place_left.wait_recv()
            place_right.wait_send()

        total = jnp.zeros((BX, BY), jnp.float32)
        cell_x = whole_iota((BX, 1), 0).astype(jnp.float32)
        cell_y = whole_iota((1, BY), 1).astype(jnp.float32)
        for number in range(places.shape[0]):
            origin_x = float((0, -BX, BX)[number // 3])
            origin_y = float((0, -BY, BY)[number % 3])
            for k in range(slots):
                start_x = places[number, k : k + 1, 0:1] + origin_x
                start_y = places[number, k : k + 1, 1:2] + origin_y
                weight = places[number, k : k + 1, 2:3]
                total += (ramp_at(cell_x - start_x, length) * weight) * ramp_at(cell_y - start_y, rows)
        scale[...] = 1.0 / jnp.maximum(total, 1.0)

    @pl.when(step >= LAG_X)
    def _():
        n = step - LAG_X

        @pl.when(has_left)
        def _():
            copy_right(n).wait_recv()
            centre[n, RX : 2 * RX] += from_left[n]
            copy_left(n).wait_send()

        @pl.when(has_right)
        def _():
            copy_left(n).wait_recv()
            centre[n, BX : BX + RX] += from_right[n]
            copy_right(n).wait_send()

        @pl.when(has_below)
        def _():
            copy_below(n).wait_send()

        @pl.when(has_above)
        def _():
            copy_above(n).wait_send()

        @pl.when(even & far_right & by_relay_right(n))
        def _():
            relay_right(n).wait_send()

        @pl.when(jnp.logical_not(even) & far_left & by_relay_left(n))
        def _():
            relay_left(n).wait_send()

        out_ref[n] = centre[n, RX : RX + BX] * scale[...]


def local(grid_x, grid_y, tiles, tile_offsets, tile_shifts, tile_counts):
    slots, count, length, rows = tiles.shape
    extent_x, extent_y = BX + 2 * RX, BY + 2 * RY
    plane = (slots, 1, length, rows)
    slab = lambda *shape: pltpu.VMEM((count,) + shape, jnp.float32)
    return pl.pallas_call(
        functools.partial(kernel, grid_x, grid_y),
        grid=(count + LAG_X,),
        in_specs=[
            pl.BlockSpec(memory_space=pltpu.SMEM),
            pl.BlockSpec(memory_space=pltpu.SMEM),
            pl.BlockSpec(memory_space=pltpu.SMEM),
            pl.BlockSpec(plane, lambda s: (0, 0, 0, 0)),
            pl.BlockSpec(plane, lambda s: (0, jnp.minimum(s + 1, count - 1), 0, 0)),
        ],
        out_specs=pl.BlockSpec(memory_space=pltpu.VMEM),
        out_shape=pltpu.VMEM((count, BX, BY), jnp.float32),
        scratch_shapes=[
            slab(extent_x, BY),
            slab(extent_x, RY),
            slab(extent_x, RY),
            slab(extent_x, RY),
            slab(extent_x, RY),
            slab(RX, BY),
            slab(RX, BY),
            slab(RX, BY),
            pltpu.VMEM((9, 8 * pl.cdiv(slots, 8), LANES), jnp.float32),
            pltpu.VMEM((extent_x, 2 * slots * length), jnp.bfloat16),
            pltpu.VMEM((slots, rows, extent_y), jnp.bfloat16),
            pltpu.VMEM((slots, length, extent_y), jnp.float32),
            pltpu.VMEM((2 * slots * length, extent_y), jnp.bfloat16),
            pltpu.VMEM((BX, BY), jnp.float32),
        ]
        + [pltpu.SemaphoreType.DMA((count,))] * 10
        + [pltpu.SemaphoreType.DMA((4,))] * 2,
        compiler_params=pltpu.CompilerParams(
            collective_id=0, has_side_effects=True, vmem_limit_bytes=52 * 1024 * 1024,
            dimension_semantics=("arbitrary",),
        ),
        name="merged",
    )(tile_offsets, tile_shifts, tile_counts, tiles, tiles)


def solution(mesh):
    placed = (
        P(("gx", "gy"), None, None, None),
        P(None, ("gx", "gy")),
        P(("gx", "gy")),
        P(("gx", "gy")),
    )
    return jax.shard_map(
        functools.partial(local, mesh.shape["gx"], mesh.shape["gy"]),
        mesh=mesh, in_specs=placed, out_specs=P(None, "gx", "gy"), check_vma=False,
    )
```
